32 devices in a mesh: dev: 32 (over z, y, x, core).
Axes of the slice: x: 2, y: 2, z: 4, core: 2. Of those that a mesh axis runs over, the one named last changes fastest.
Arguments:
- source: bfloat16 [48, 262144], P(None, 'dev'), may hold values from -6 to 6
- weights: bfloat16 [20480, 128, 128], P('dev'), may hold values from -0.01953125 to 0.01953125
- tile_map: int32 [3, 20480], P(None, 'dev'), may hold values from 0 to 63, as said below
- tile_count: int32 [32], P('dev'), may hold values from 160 to 640, as said below
Outputs:
- acoustic_source: float32 [48, 4096], P(None, 'dev')
The draws below stay inside these ranges and needn't reach their ends.
Inputs may be any that keep to these rules, and one draw needn't show every extreme that they name: `tile_map`: row 0 is a CFD block of the owning device; row 2 an acoustic block of the destination. Row 1 is a device at cyclic distance at most 4 from the owner in device order, or at distance exactly 32 // 2 (counted upward); every device has used slots at distance +4, -4 and 32 // 2. `tile_count`: some device uses all its slots.
All inputs are finite; a program needn't handle non-finite values.
Results may differ from the reference program's by a relative error of at most 0.0003.
Values sent between devices are 32-bit elements; how exact they have to be, the bound alone decides.
A program may use at most 128 MiB of HBM per device.

```python
import jax
import jax.numpy as jnp
from jax import lax

BLK = 128
REACH = 4
SRC_BLK_DEV = 64
TILES_DEV = 640
ACU_BLK_DEV = 1
FEAT = 48
CELLS = 262144
TILES = 20480
N_DEV = 32


def draw_tile_map(key, part):
    key_src = jax.random.fold_in(key, 11)
    key_off = jax.random.fold_in(key, 12)
    key_blk = jax.random.fold_in(key, 13)
    total = N_DEV * TILES_DEV
    src_ids = jax.random.randint(key_src, (total,), 0, SRC_BLK_DEV)
    offsets = jax.random.randint(key_off, (total,), -REACH, REACH + 1)
    slot = jnp.arange(total) % TILES_DEV
    offsets = jnp.where(slot == 0, REACH, jnp.where(slot == 1, -REACH, jnp.where(slot == 2, N_DEV // 2, offsets)))
    owner = jnp.arange(total) // TILES_DEV
    dest = (owner + offsets) % N_DEV
    dest_blk = jax.random.randint(key_blk, (total,), 0, ACU_BLK_DEV)
    return jnp.stack([src_ids, dest, dest_blk]).astype(jnp.int32)


def draw_tile_count(key, part):
    key_cnt = jax.random.fold_in(key, 21)
    key_full = jax.random.fold_in(key, 22)
    lowest = max(TILES_DEV // 4, 3)
    counts = jax.random.randint(key_cnt, (N_DEV,), lowest, TILES_DEV + 1)
    busiest = jax.random.randint(key_full, (), 0, N_DEV)
    counts = jnp.where(jnp.arange(N_DEV) == busiest, TILES_DEV, counts)
    return counts.astype(jnp.int32)


def block_scale(own_key, shape, cuts, low, high):
    level = 1.0
    for position, shards_of in cuts:
        steps = jax.random.uniform(jax.random.fold_in(jax.random.fold_in(own_key, 6), position), (shards_of,), jnp.float32, low / len(cuts), high / len(cuts))
        level = level * jnp.repeat(jnp.exp(steps), shape[position] // shards_of).reshape((-1,) + (1,) * (len(shape) - 1 - position))
    return level


def centred(own_key, dims, scale, most, split=(), kind=jnp.bfloat16):
    drawn = jax.random.normal(own_key, dims, jnp.float32) * scale
    if len(split) > 0:
        drawn = block_scale(own_key, dims, split, -0.22, 0.18) * drawn
    return jnp.clip(drawn, min=-most, max=most).astype(kind)


def setup_inputs(seed: int = 0) -> dict:
    splits = jax.random.split(jax.random.key(seed), 5)
    source = centred(splits[0], (FEAT, CELLS), 1.0, 6.0, ((1, 32),))
    weights = centred(splits[1], (TILES, BLK, BLK), (BLK * TILES_DEV // ACU_BLK_DEV) ** -0.5, 0.01953125, ((0, 32),))
    tile_map = draw_tile_map(jax.random.fold_in(splits[4], 71), 0)
    tile_count = draw_tile_count(jax.random.fold_in(splits[4], 71), 0)
    return dict(source=source, weights=weights, tile_map=tile_map, tile_count=tile_count)


def reference(source, weights, tile_map, tile_count):
    feat = source.shape[0]
    blocks = source.reshape(feat, N_DEV * SRC_BLK_DEV, BLK).astype(jnp.float32)

    def one_device(acc, device):
        start = device * TILES_DEV
        tile_w = lax.dynamic_slice_in_dim(weights, start, TILES_DEV, 0).astype(jnp.float32)
        mapped = lax.dynamic_slice_in_dim(tile_map, start, TILES_DEV, 1)
        block_ids = (device * SRC_BLK_DEV + mapped[0]).astype(jnp.int32)
        picked = jnp.take(blocks, block_ids, axis=1)
        product = jnp.einsum("ftc,tcn->tfn", picked, tile_w, precision=lax.Precision.HIGHEST)
        used = (jnp.arange(TILES_DEV, dtype=jnp.int32) < tile_count[device]).astype(jnp.float32)
        product = product * used[:, None, None]
        target = (mapped[1] * ACU_BLK_DEV + mapped[2]).astype(jnp.int32)
        return acc.at[target].add(product), None

    start_acc = jnp.zeros((N_DEV * ACU_BLK_DEV, feat, BLK), jnp.float32)
    acc, _ = lax.scan(one_device, start_acc, jnp.arange(N_DEV, dtype=jnp.int32))
    return jnp.transpose(acc, (1, 0, 2)).reshape(feat, N_DEV * ACU_BLK_DEV * BLK)
```

```python
import functools

import jax
import jax.numpy as jnp
from jax import lax
from jax.experimental import pallas as pl
from jax.experimental.pallas import tpu as pltpu
from jax.sharding import PartitionSpec as P

REACH = 4
ACU_BLK_DEV = 1
CHUNK = 32
COPIES = 8


def passed_along(value, axis, steps):
    count = lax.axis_size(axis)
    pairs = [(source, (source + steps) % count) for source in range(count)]
    return lax.ppermute(value, axis, pairs)


def sums_kernel(devices, chunk, map_ref, count_ref, src_hbm, w_hbm, out_ref, src, w, lut, src_sem, w_sem, *accs):
    tiles, blk, _ = w_hbm.shape
    slots = out_ref.shape[0]
    own = lax.axis_index("dev")
    count = count_ref[0]
    trips = lax.div(count + (chunk - 1), chunk)

    def chunk_copy(c):
        rows = pl.ds(pl.multiple_of(c * chunk, chunk), chunk)
        return pltpu.make_async_copy(w_hbm.at[rows], w.at[rows], w_sem.at[c])

    src_copy = pltpu.make_async_copy(src_hbm, src, src_sem)
    src_copy.start()

    @pl.loop(0, trips)
    def _(c):
        chunk_copy(c).start()

    for slot in range(2 * REACH + 1):
        lut[lax.rem(own + (slot - REACH) + devices, devices)] = slot
    if devices // 2 > REACH:
        lut[lax.rem(own + devices // 2, devices)] = 2 * REACH + 1

    for acc in accs:
        acc[...] = jnp.zeros_like(acc)
    src_copy.wait()

    @pl.loop(0, trips)
    def _(c):
        chunk_copy(c).wait()
        for j in range(chunk):
            t = c * chunk + j
            begin = pl.multiple_of(map_ref[0, t] * blk, blk)
            key = lut[map_ref[1, t]]
            if ACU_BLK_DEV > 1:
                key = key * ACU_BLK_DEV + map_ref[2, t]
            key = jnp.where(t < count, key, slots)
            product = jnp.dot(src[:, pl.ds(begin, blk)], w[t], preferred_element_type=jnp.float32)
            acc = accs[j % len(accs)]
            acc[key] += product

    for slot in range(slots):
        total = accs[0][slot]
        for acc in accs[1:]:
            total = total + acc[slot]
        out_ref[slot] = total


def local_sums(source, weights, tile_map, tile_count):
    feat = source.shape[0]
    tiles, blk, _ = weights.shape
    devices = lax.axis_size("dev")
    chunk = CHUNK
    while tiles % chunk:
        chunk //= 2
    slots = (2 * REACH + 2) * ACU_BLK_DEV
    return pl.pallas_call(
        functools.partial(sums_kernel, devices, chunk),
        out_shape=jax.ShapeDtypeStruct((slots, feat, blk), jnp.float32),
        in_specs=[
            pl.BlockSpec(memory_space=pltpu.SMEM),
            pl.BlockSpec(memory_space=pltpu.SMEM),
            pl.BlockSpec(memory_space=pl.ANY),
            pl.BlockSpec(memory_space=pl.ANY),
        ],
        out_specs=pl.BlockSpec(memory_space=pltpu.VMEM),
        scratch_shapes=[
            pltpu.VMEM(source.shape, source.dtype),
            pltpu.VMEM(weights.shape, weights.dtype),
            pltpu.SMEM((devices,), jnp.int32),
            pltpu.SemaphoreType.DMA,
            pltpu.SemaphoreType.DMA((tiles // chunk,)),
        ]
        + [pltpu.VMEM((slots + 1, feat, blk), jnp.float32) for _ in range(COPIES)],
        name="local_sums",
    )(tile_map, tile_count, source, weights)


def on_device(source, weights, tile_map, tile_count):
    feat = source.shape[0]
    blk = weights.shape[1]
    acu = ACU_BLK_DEV
    devices = lax.axis_size("dev")
    far_slot = 2 * REACH + 1
    outgoing = local_sums(source, weights, tile_map, tile_count)
    outgoing = outgoing.reshape(2 * REACH + 2, acu, feat, blk)
    total = outgoing[REACH]
    for index in range(2 * REACH + 1):
        if index != REACH:
            total = total + passed_along(outgoing[index], "dev", index - REACH)
    total = total + passed_along(outgoing[far_slot], "dev", devices // 2)
    return jnp.transpose(total, (1, 0, 2)).reshape(feat, acu * blk)


def solution(mesh):
    return jax.shard_map(
        on_device,
        mesh=mesh,
        in_specs=(P(None, "dev"), P("dev", None, None), P(None, "dev"), P("dev")),
        out_specs=P(None, "dev"),
        check_vma=False,
    )
```

```python
import functools

import jax
import jax.numpy as jnp
from jax import lax
from jax.experimental import pallas as pl
from jax.experimental.pallas import tpu as pltpu
from jax.sharding import PartitionSpec as P

REACH = 4
ACU_BLK_DEV = 1
CHUNK = 32
COPIES = 8


def near_and_far(devices):
    pairs = []
    if devices // 2 > REACH:
        pairs.append((devices // 2, 2 * REACH + 1))
    for step in range(REACH, 0, -1):
        pairs += [(step, REACH + step), (-step, REACH - step)]
    return pairs


def exchange_kernel(devices, sums, out_ref, landed, send_sem, recv_sem):
    acu = ACU_BLK_DEV
    own = lax.axis_index("dev")
    pairs = near_and_far(devices)
    barrier = pltpu.get_barrier_semaphore()
    for distance, _ in pairs:
        pl.semaphore_signal(
            barrier,
            inc=1,
            device_id=(lax.rem(own - distance + devices, devices),),
            device_id_type=pl.DeviceIdType.MESH,
        )
    pl.semaphore_wait(barrier, len(pairs))
    copies = []
    for index, (distance, slot) in enumerate(pairs):
        copies.append(
            pltpu.make_async_remote_copy(
                src_ref=sums.at[pl.ds(slot * acu, acu)],
                dst_ref=landed.at[index],
                send_sem=send_sem.at[index],
                recv_sem=recv_sem.at[index],
                device_id=(lax.rem(own + distance + devices, devices),),
                device_id_type=pl.DeviceIdType.MESH,
            )
        )
        copies[-1].start()
    total = sums[pl.ds(REACH * acu, acu)]
    for index in reversed(range(len(pairs))):
        copies[index].wait_recv()
        total = total + landed[index]
    out_ref[...] = total
    for copy in copies:
        copy.wait_send()


def exchanged(sums):
    devices = lax.axis_size("dev")
    _, feat, blk = sums.shape
    flows = len(near_and_far(devices))
    return pl.pallas_call(
        functools.partial(exchange_kernel, devices),
        out_shape=jax.ShapeDtypeStruct((ACU_BLK_DEV, feat, blk), jnp.float32),
        in_specs=[pl.BlockSpec(memory_space=pltpu.VMEM)],
        out_specs=pl.BlockSpec(memory_space=pltpu.VMEM),
        scratch_shapes=[
            pltpu.VMEM((flows, ACU_BLK_DEV, feat, blk), jnp.float32),
            pltpu.SemaphoreType.DMA((flows,)),
            pltpu.SemaphoreType.DMA((flows,)),
        ],
        compiler_params=pltpu.CompilerParams(collective_id=0, has_side_effects=True),
        name="exchange",
    )(sums)


def sums_kernel(devices, chunk, map_ref, count_ref, src_hbm, w_hbm, out_ref, src, w, lut, src_sem, w_sem, *accs):
    tiles, blk, _ = w_hbm.shape
    slots = out_ref.shape[0]
    own = lax.axis_index("dev")
    count = count_ref[0]
    trips = lax.div(count + (chunk - 1), chunk)

    def chunk_copy(c):
        rows = pl.ds(pl.multiple_of(c * chunk, chunk), chunk)
        return pltpu.make_async_copy(w_hbm.at[rows], w.at[rows], w_sem.at[c])

    src_copy = pltpu.make_async_copy(src_hbm, src, src_sem)
    src_copy.start()

    @pl.loop(0, trips)
    def _(c):
        chunk_copy(c).start()

    for slot in range(2 * REACH + 1):
        lut[lax.rem(own + (slot - REACH) + devices, devices)] = slot
    if devices // 2 > REACH:
        lut[lax.rem(own + devices // 2, devices)] = 2 * REACH + 1

    for acc in accs:
        acc[...] = jnp.zeros_like(acc)
    src_copy.wait()

    @pl.loop(0, trips)
    def _(c):
        chunk_copy(c).wait()
        for j in range(chunk):
            t = c * chunk + j
            begin = pl.multiple_of(map_ref[0, t] * blk, blk)
            key = lut[map_ref[1, t]]
            if ACU_BLK_DEV > 1:
                key = key * ACU_BLK_DEV + map_ref[2, t]
            key = jnp.where(t < count, key, slots)
            product = jnp.dot(src[:, pl.ds(begin, blk)], w[t], preferred_element_type=jnp.float32)
            acc = accs[j % len(accs)]
            acc[key] += product

    for slot in range(slots):
        total = accs[0][slot]
        for acc in accs[1:]:
            total = total + acc[slot]
        out_ref[slot] = total


def local_sums(source, weights, tile_map, tile_count):
    feat = source.shape[0]
    tiles, blk, _ = weights.shape
    devices = lax.axis_size("dev")
    chunk = CHUNK
    while tiles % chunk:
        chunk //= 2
    slots = (2 * REACH + 2) * ACU_BLK_DEV
    return pl.pallas_call(
        functools.partial(sums_kernel, devices, chunk),
        out_shape=jax.ShapeDtypeStruct((slots, feat, blk), jnp.float32),
        in_specs=[
            pl.BlockSpec(memory_space=pltpu.SMEM),
            pl.BlockSpec(memory_space=pltpu.SMEM),
            pl.BlockSpec(memory_space=pl.ANY),
            pl.BlockSpec(memory_space=pl.ANY),
        ],
        out_specs=pl.BlockSpec(memory_space=pltpu.VMEM),
        scratch_shapes=[
            pltpu.VMEM(source.shape, source.dtype),
            pltpu.VMEM(weights.shape, weights.dtype),
            pltpu.SMEM((devices,), jnp.int32),
            pltpu.SemaphoreType.DMA,
            pltpu.SemaphoreType.DMA((tiles // chunk,)),
        ]
        + [pltpu.VMEM((slots + 1, feat, blk), jnp.float32) for _ in range(COPIES)],
        name="local_sums",
    )(tile_map, tile_count, source, weights)


def on_device(source, weights, tile_map, tile_count):
    feat = source.shape[0]
    blk = weights.shape[1]
    acu = ACU_BLK_DEV
    total = exchanged(local_sums(source, weights, tile_map, tile_count))
    return jnp.transpose(total, (1, 0, 2)).reshape(feat, acu * blk)


def solution(mesh):
    return jax.shard_map(
        on_device,
        mesh=mesh,
        in_specs=(P(None, "dev"), P("dev", None, None), P(None, "dev"), P("dev")),
        out_specs=P(None, "dev"),
        check_vma=False,
    )
```
